64 devices in a mesh: dp: 4 (over x, y), cp: 16 (over z, core).
Axes of the slice: x: 2, y: 2, z: 8, core: 2. Of those that a mesh axis runs over, the one named last changes fastest.
The devices are a block of a 4x4x8 slice.
Arguments:
- query: bfloat16 [64, 1024, 16, 128], P('dp', 'cp'), parts along dimension 0
- keys: bfloat16 [64, 1024, 1, 128], P('dp', 'cp'), parts along dimension 0
- values: bfloat16 [64, 1024, 1, 128], P('dp', 'cp'), parts along dimension 0
- grad_out: bfloat16 [64, 1024, 16, 128], P('dp', 'cp'), parts along dimension 0
- doc_id: int32 [64, 1024], P('dp', 'cp'), parts along dimension 0
Outputs:
- output 1: bfloat16 [64, 1024, 16, 128], P('dp', 'cp'), parts along dimension 0
- output 2: bfloat16 [64, 1024, 16, 128], P('dp', 'cp'), parts along dimension 0
- output 3: bfloat16 [64, 1024, 1, 128], P('dp', 'cp'), parts along dimension 0
- output 4: bfloat16 [64, 1024, 1, 128], P('dp', 'cp'), parts along dimension 0
There are 4 independent parts. The reference program is written for one: setup_inputs(seed, part) draws one part's arguments, and reference() takes and returns one part's arrays. A program takes and returns all parts, laid end to end along the dimension named above; each array names one.
All inputs are finite; a program needn't handle non-finite values.
Results may differ from the reference program's by a relative error of at most 0.0108808.
Values are sent between devices in bfloat16 or wider.
A program may use at most 768 MiB of HBM per device.

```python
import jax
import jax.numpy as jnp
from jax import lax

BATCH = 16
SEQ = 1024
HEADS = 16
HEAD = 128
ROW_BLOCK = 4
DOC_CUTS = 4
NEG_BIG = -1e30


def doc_ids_row(key):
    key_cut, key_count = jax.random.split(key)
    cut_pos = jax.random.permutation(key_cut, SEQ - 1)[:DOC_CUTS] + 1
    cut_count = jax.random.randint(key_count, (), 1, DOC_CUTS + 1)
    cut_valid = jnp.arange(DOC_CUTS) < cut_count
    positions = jnp.arange(SEQ)
    cut_hits = (cut_pos[None, :] <= positions[:, None]) & cut_valid[None, :]
    return jnp.sum(cut_hits.astype(jnp.int32), axis=1).astype(jnp.int32)


def setup_inputs(seed: int = 0, part: int = 0) -> dict:
    key = jax.random.fold_in(jax.random.key(seed), part)
    key_q, key_k, key_v, key_slow, key_g, key_doc = jax.random.split(key, 6)
    query = 1.5 * jax.random.normal(key_q, (BATCH, SEQ, HEADS, HEAD), jnp.float32)
    keys = 1.5 * jax.random.normal(key_k, (BATCH, SEQ, 1, HEAD), jnp.float32)
    slow = jax.random.normal(key_slow, (BATCH, 16, 1, HEAD), jnp.float32)
    noise = jax.random.normal(key_v, (BATCH, SEQ, 1, HEAD), jnp.float32)
    values = 0.8 * jnp.repeat(slow, SEQ // 16, axis=1) + 0.6 * noise
    grad_out = 0.5 * jax.random.normal(key_g, (BATCH, SEQ, HEADS, HEAD), jnp.float32)
    doc_id = jax.vmap(doc_ids_row)(jax.random.split(key_doc, BATCH))
    return {'query': query.astype(jnp.bfloat16), 'keys': keys.astype(jnp.bfloat16), 'values': values.astype(jnp.bfloat16), 'grad_out': grad_out.astype(jnp.bfloat16), 'doc_id': doc_id}


def reference(query, keys, values, grad_out, doc_id):
    score_scale = HEAD ** -0.5
    n_blocks = SEQ // ROW_BLOCK
    key_pos = jnp.arange(SEQ)
    pos_blocks = key_pos.reshape(n_blocks, ROW_BLOCK)

    def one_row(row):
        q_row, k_row, v_row, g_row, doc_row = row
        k_mat = k_row[:, 0, :].astype(jnp.float32)
        v_mat = v_row[:, 0, :].astype(jnp.float32)
        q_blocks = q_row.reshape(n_blocks, ROW_BLOCK, HEADS, HEAD)
        g_blocks = g_row.reshape(n_blocks, ROW_BLOCK, HEADS, HEAD)
        doc_blocks = doc_row.reshape(n_blocks, ROW_BLOCK)

        def step(carry, block):
            dk_acc, dv_acc = carry
            q_block, g_block, doc_block, pos_block = block
            q_wide = q_block.astype(jnp.float32)
            g_wide = g_block.astype(jnp.float32)
            visible = (key_pos[None, :] <= pos_block[:, None]) & (doc_row[None, :] == doc_block[:, None])
            raw_scores = jnp.einsum('qhd,kd->qhk', q_wide, k_mat) * score_scale
            scores = jnp.where(visible[:, None, :], raw_scores, NEG_BIG)
            exp_scores = jnp.exp(scores - jnp.max(scores, axis=-1, keepdims=True))
            prob_f32 = exp_scores / jnp.sum(exp_scores, axis=-1, keepdims=True)
            prob_low = prob_f32.astype(jnp.bfloat16).astype(jnp.float32)
            out_block = jnp.einsum('qhk,kd->qhd', prob_low, v_mat).astype(jnp.bfloat16)
            row_delta = jnp.einsum('qhd,qhd->qh', g_wide, out_block.astype(jnp.float32))
            grad_prob = jnp.einsum('qhd,kd->qhk', g_wide, v_mat)
            grad_score = (prob_f32 * (grad_prob - row_delta[:, :, None])).astype(jnp.bfloat16).astype(jnp.float32)
            dq_block = (jnp.einsum('qhk,kd->qhd', grad_score, k_mat) * score_scale).astype(jnp.bfloat16)
            dk_acc = dk_acc + jnp.einsum('qhk,qhd->kd', grad_score, q_wide)
            dv_acc = dv_acc + jnp.einsum('qhk,qhd->kd', prob_low, g_wide)
            return (dk_acc, dv_acc), (out_block, dq_block)

        kv_zero = jnp.zeros((SEQ, HEAD), jnp.float32)
        sums, blocks = lax.scan(step, (kv_zero, kv_zero), (q_blocks, g_blocks, doc_blocks, pos_blocks))
        out_row = blocks[0].reshape(SEQ, HEADS, HEAD)
        dq_row = blocks[1].reshape(SEQ, HEADS, HEAD)
        dk_row = (sums[0] * score_scale).astype(jnp.bfloat16)[:, None, :]
        dv_row = sums[1].astype(jnp.bfloat16)[:, None, :]
        return out_row, dq_row, dk_row, dv_row

    attn_out, grad_query, grad_keys, grad_values = lax.map(one_row, (query, keys, values, grad_out, doc_id))
    return (attn_out, grad_query, grad_keys, grad_values)
```

```python
import functools

import jax
import jax.numpy as jnp
from jax import lax
from jax.experimental import pallas as pl
from jax.experimental.pallas import tpu as pltpu
from jax.sharding import PartitionSpec as P

LOG2E = 1.4426950408889634
MASKED = -3e38
UNMASKED = 3e38
KEY_BLOCK = 256
ROW_BLOCK = 256
NT = (((1,), (1,)), ((), ()))


def attention_kernel(n_chunk, meta, q_ref, g_ref, kv_ref, doc_row_ref, doc_col_ref, o_ref, dq_ref, dkv_ref,
                     s_scr, stat_scr, inv_scr, acc_scr, p_scr, ds_scr, qt_scr, gt_scr):
    b = pl.program_id(0)
    n_dev, _, piece, wide = kv_ref.shape
    head_dim = wide // 2
    n_heads = q_ref.shape[2]
    rows = piece * n_heads
    per_block = KEY_BLOCK // piece
    n_blocks = n_dev * piece // KEY_BLOCK
    n_rows = rows // ROW_BLOCK
    toks = ROW_BLOCK // n_heads
    scale = head_dim ** -0.5
    lo = meta[b]
    rank = meta[n_chunk]
    hi = (rank * piece + piece + KEY_BLOCK - 1) // KEY_BLOCK
    f32 = jnp.float32
    bf16 = jnp.bfloat16

    def load_rows(ref, c):
        return ref[0, c * toks:(c + 1) * toks].reshape(ROW_BLOCK, head_dim)

    def keys_at(kb):
        blk = kv_ref[pl.ds(kb * per_block, per_block), 0, :, :head_dim]
        return blk.reshape(KEY_BLOCK, head_dim)

    def vals_at(kb):
        blk = kv_ref[pl.ds(kb * per_block, per_block), 0, :, head_dim:]
        return blk.reshape(KEY_BLOCK, head_dim)

    for c in range(n_rows):
        sl = slice(c * ROW_BLOCK, (c + 1) * ROW_BLOCK)
        qt_scr[:, sl] = load_rows(q_ref, c).T
        gt_scr[:, sl] = load_rows(g_ref, c).T

    stat_scr[...] = jnp.full(stat_scr.shape, MASKED, f32)

    def score_step(kb, carry):
        key = keys_at(kb)
        col = kb * KEY_BLOCK + lax.broadcasted_iota(jnp.int32, (piece, KEY_BLOCK), 1)
        row = rank * piece + lax.broadcasted_iota(jnp.int32, (piece, KEY_BLOCK), 0)
        doc_k = doc_row_ref[0, :, pl.ds(kb * KEY_BLOCK, KEY_BLOCK)]
        doc_q = doc_col_ref[0]
        doc_q = jnp.concatenate([doc_q] * (KEY_BLOCK // doc_q.shape[1]), axis=1)
        visible = (col <= row) & (doc_q == doc_k)
        limit = jnp.where(visible, UNMASKED, MASKED)
        for c in range(n_rows):
            sl = slice(c * ROW_BLOCK, (c + 1) * ROW_BLOCK)
            raw = lax.dot_general(load_rows(q_ref, c), key, NT, preferred_element_type=f32)
            lim = limit[c * toks:(c + 1) * toks]
            raw = jnp.minimum(raw.reshape(toks, n_heads, KEY_BLOCK), lim[:, None, :]).reshape(ROW_BLOCK, KEY_BLOCK)
            s_scr[kb, sl, :] = raw
            top = stat_scr[sl]
            for p in range(KEY_BLOCK // 128):
                top = jnp.maximum(top, raw[:, p * 128:(p + 1) * 128])
            stat_scr[sl] = top
        return carry

    lax.fori_loop(lo, hi, score_step, 0)
    for c in range(n_rows):
        sl = slice(c * ROW_BLOCK, (c + 1) * ROW_BLOCK)
        stat_scr[sl] = jnp.broadcast_to(jnp.max(stat_scr[sl], axis=1, keepdims=True), (ROW_BLOCK, 128))
    inv_scr[...] = jnp.zeros(inv_scr.shape, f32)

    def exp_step(kb, carry):
        for c in range(n_rows):
            sl = slice(c * ROW_BLOCK, (c + 1) * ROW_BLOCK)
            top = stat_scr[sl]
            total = inv_scr[sl]
            for p in range(KEY_BLOCK // 128):
                lanes = slice(p * 128, (p + 1) * 128)
                e = jnp.exp2((s_scr[kb, sl, lanes] - top) * (scale * LOG2E))
                s_scr[kb, sl, lanes] = e
                total = total + e
            inv_scr[sl] = total
        return carry

    lax.fori_loop(lo, hi, exp_step, 0)
    for c in range(n_rows):
        sl = slice(c * ROW_BLOCK, (c + 1) * ROW_BLOCK)
        inv_scr[sl] = jnp.broadcast_to(1.0 / jnp.sum(inv_scr[sl], axis=1, keepdims=True), (ROW_BLOCK, 128))
    acc_scr[...] = jnp.zeros(acc_scr.shape, f32)

    def out_step(kb, carry):
        val = vals_at(kb)
        for c in range(n_rows):
            sl = slice(c * ROW_BLOCK, (c + 1) * ROW_BLOCK)
            inv = inv_scr[sl]
            parts = []
            for p in range(KEY_BLOCK // 128):
                lanes = slice(p * 128, (p + 1) * 128)
                prob = s_scr[kb, sl, lanes] * inv
                s_scr[kb, sl, lanes] = prob
                parts.append(prob.astype(bf16))
            acc_scr[sl] += jnp.dot(jnp.concatenate(parts, axis=1), val, preferred_element_type=f32)
        return carry

    lax.fori_loop(lo, hi, out_step, 0)
    for c in range(n_rows):
        sl = slice(c * ROW_BLOCK, (c + 1) * ROW_BLOCK)
        out = acc_scr[sl].astype(bf16)
        o_ref[0, c * toks:(c + 1) * toks] = out.reshape(toks, n_heads, head_dim)
        delta = jnp.sum(load_rows(g_ref, c).astype(f32) * out.astype(f32), axis=1, keepdims=True)
        stat_scr[sl] = jnp.broadcast_to(delta, (ROW_BLOCK, 128))
    acc_scr[...] = jnp.zeros(acc_scr.shape, f32)

    def grad_step(kb, carry):
        key = keys_at(kb)
        val = vals_at(kb)
        for c in range(n_rows):
            sl = slice(c * ROW_BLOCK, (c + 1) * ROW_BLOCK)
            gp = lax.dot_general(load_rows(g_ref, c), val, NT, preferred_element_type=f32)
            delta = stat_scr[sl]
            parts = []
            for p in range(KEY_BLOCK // 128):
                lanes = slice(p * 128, (p + 1) * 128)
                prob = s_scr[kb, sl, lanes]
                p_scr[sl, lanes] = prob.astype(bf16)
                parts.append((prob * (gp[:, lanes] - delta)).astype(bf16))
            ds = jnp.concatenate(parts, axis=1)
            ds_scr[sl, :] = ds
            acc_scr[sl] += jnp.dot(ds, key, preferred_element_type=f32)
        dk_t = jnp.dot(qt_scr[...], ds_scr[...], preferred_element_type=f32)
        dv_t = jnp.dot(gt_scr[...], p_scr[...], preferred_element_type=f32)
        dkv_ref[pl.ds(kb * per_block, per_block), 0, :, :head_dim] = dk_t.T.reshape(per_block, piece, head_dim)
        dkv_ref[pl.ds(kb * per_block, per_block), 0, :, head_dim:] = dv_t.T.reshape(per_block, piece, head_dim)
        return carry

    lax.fori_loop(lo, hi, grad_step, 0)
    for c in range(n_rows):
        sl = slice(c * ROW_BLOCK, (c + 1) * ROW_BLOCK)
        dq_ref[0, c * toks:(c + 1) * toks] = (acc_scr[sl] * scale).astype(bf16).reshape(toks, n_heads, head_dim)

    def zero_step(kb, carry):
        dkv_ref[pl.ds(kb * per_block, per_block)] = jnp.zeros((per_block, 1, piece, wide), f32)
        return carry

    lax.fori_loop(0, lo, zero_step, 0)
    lax.fori_loop(hi, n_blocks, zero_step, 0)


def attention(query, grad_out, kv_all, doc_all, doc_loc, rank):
    n_dev, n_chunk, piece, wide = kv_all.shape
    n_heads, head_dim = query.shape[2:]
    rows = piece * n_heads
    seq = n_dev * piece
    first = jnp.sum((doc_all < doc_loc[:, :1]).astype(jnp.int32), axis=1)
    meta = jnp.concatenate([first // KEY_BLOCK, rank[None].astype(jnp.int32)])
    doc_row = doc_all[:, None, :]
    doc_col = jnp.broadcast_to(doc_loc[:, :, None], (n_chunk, piece, 128))
    tok_spec = pl.BlockSpec((1, piece, n_heads, head_dim), lambda b, m: (b, 0, 0, 0))
    kv_spec = pl.BlockSpec((n_dev, 1, piece, wide), lambda b, m: (0, b, 0, 0))
    f32 = jnp.float32
    bf16 = jnp.bfloat16
    return pl.pallas_call(
        functools.partial(attention_kernel, n_chunk),
        grid_spec=pltpu.PrefetchScalarGridSpec(
            num_scalar_prefetch=1,
            grid=(n_chunk,),
            in_specs=[tok_spec, tok_spec, kv_spec,
                      pl.BlockSpec((1, 1, seq), lambda b, m: (b, 0, 0)),
                      pl.BlockSpec((1, piece, 128), lambda b, m: (b, 0, 0))],
            out_specs=[tok_spec, tok_spec, kv_spec],
            scratch_shapes=[
                pltpu.VMEM((seq // KEY_BLOCK, rows, KEY_BLOCK), f32),
                pltpu.VMEM((rows, 128), f32),
                pltpu.VMEM((rows, 128), f32),
                pltpu.VMEM((rows, head_dim), f32),
                pltpu.VMEM((rows, KEY_BLOCK), bf16),
                pltpu.VMEM((rows, KEY_BLOCK), bf16),
                pltpu.VMEM((head_dim, rows), bf16),
                pltpu.VMEM((head_dim, rows), bf16),
            ]),
        out_shape=[jax.ShapeDtypeStruct(query.shape, bf16),
                   jax.ShapeDtypeStruct(query.shape, bf16),
                   jax.ShapeDtypeStruct((n_dev, n_chunk, piece, wide), f32)],
        cost_estimate=pl.CostEstimate(
            flops=6 * n_chunk * rows * seq * head_dim,
            bytes_accessed=4 * query.size * 2 + kv_all.size * 6,
            transcendentals=n_chunk * rows * seq // 2),
    )(meta, query, grad_out, kv_all, doc_row, doc_col)


def solution(mesh):
    seq_spec = P('dp', 'cp', None, None)
    id_spec = P('dp', 'cp')

    def per_device(query, keys, values, grad_out, doc_id):
        head_dim = query.shape[3]
        rank = lax.axis_index('cp')
        kv_loc = jnp.concatenate([keys[:, :, 0, :], values[:, :, 0, :]], axis=-1)
        kv_all = lax.all_gather(kv_loc, 'cp')
        doc_all = lax.all_gather(doc_id, 'cp', axis=1, tiled=True)
        out, grad_query, dkv = attention(query, grad_out, kv_all, doc_all, doc_id, rank)
        total = lax.psum_scatter(dkv, 'cp', scatter_dimension=0)
        grad_keys = (total[:, :, :head_dim] * head_dim ** -0.5).astype(jnp.bfloat16)[:, :, None, :]
        grad_values = total[:, :, head_dim:].astype(jnp.bfloat16)[:, :, None, :]
        return out, grad_query, grad_keys, grad_values

    return jax.shard_map(per_device, mesh=mesh, in_specs=(seq_spec, seq_spec, seq_spec, seq_spec, id_spec), out_specs=(seq_spec, seq_spec, seq_spec, seq_spec), check_vma=False)
```

```python
import functools

import jax
import jax.numpy as jnp
from jax import lax
from jax.experimental import pallas as pl
from jax.experimental.pallas import tpu as pltpu
from jax.sharding import PartitionSpec as P

LOG2E = 1.4426950408889634
MASKED = -3e38
UNMASKED = 3e38
KEY_BLOCK = 256
MESH = pl.DeviceIdType.MESH


def fused_kernel(q_ref, g_ref, kv_ref, doc_ref, doc_col_ref, o_ref, dq_ref, dkv_ref,
                 kv_all, doc_all, part, pair_in, down_in, up_in, last_in, swap_out, swap_in,
                 s_scr, stat_scr, inv_scr, acc_scr, p_scr, ds_scr, qt_scr, gt_scr,
                 g_send, g_recv, f_send, f_recv, d_send, d_recv, x_send, x_recv,
                 dn_send, dn_recv, up_send, up_recv, last_recv, sw_send, sw_recv):
    t = pl.program_id(0)
    n_seq, n_dev, piece, wide = kv_all.shape
    head_dim = wide // 2
    n_heads = q_ref.shape[2]
    rows = piece * n_heads
    row_block = min(rows, 512)
    n_rows = rows // row_block
    toks = row_block // n_heads
    per_block = KEY_BLOCK // piece
    scale = head_dim ** -0.5
    base = scale * LOG2E
    n_chip = n_dev // 2
    half = n_chip // 2
    f32 = jnp.float32
    bf16 = jnp.bfloat16
    rank = lax.axis_index('cp')
    chip = rank // 2
    core = rank % 2
    partner = chip * 2 + (1 - core)
    hi = (rank * piece + piece + KEY_BLOCK - 1) // KEY_BLOCK

    def lane_of(other):
        return other * 2 + core

    def rcopy(src, dst, ssem, rsem, dev):
        return pltpu.make_async_remote_copy(src_ref=src, dst_ref=dst, send_sem=ssem, recv_sem=rsem,
                                            device_id={'cp': dev}, device_id_type=MESH)

    def each(lower, upper, body):
        def step(i, carry):
            body(i)
            return carry
        lax.fori_loop(lower, upper, step, 0)

    def own_send(b, dst_chip, slot):
        return rcopy(kv_ref.at[b], kv_all.at[b, rank], g_send.at[b, slot], g_recv.at[b, chip], lane_of(dst_chip))

    def pass_on(b, src_chip, dst_chip):
        piece_ref = kv_all.at[b, lane_of(src_chip)]
        return rcopy(piece_ref, piece_ref, g_send.at[b, src_chip], g_recv.at[b, src_chip], lane_of(dst_chip))

    def gather_arrival(b, src_chip):
        slot = kv_all.at[b, lane_of(src_chip)]
        return rcopy(slot, slot, g_send.at[b, src_chip], g_recv.at[b, src_chip], partner)

    def forward_copy(b, src_chip):
        slot = kv_all.at[b, lane_of(src_chip)]
        return rcopy(slot, slot, f_send.at[b, src_chip], f_recv.at[b, src_chip], partner)

    def own_copy(b):
        return rcopy(kv_ref.at[b], kv_all.at[b, rank], f_send.at[b, chip], f_recv.at[b, chip], partner)

    def forward_arrival(b, src_chip):
        slot = kv_all.at[b, src_chip * 2 + (1 - core)]
        return rcopy(slot, slot, f_send.at[b, src_chip], f_recv.at[b, src_chip], partner)

    def doc_copy(dst):
        return rcopy(doc_ref, doc_all.at[rank], d_send.at[dst], d_recv.at[rank], dst)

    def doc_arrival(src):
        return rcopy(doc_ref, doc_all.at[src], d_send.at[src], d_recv.at[src], partner)

    def pair_copy(b):
        return rcopy(part.at[1 - core], pair_in.at[b], x_send.at[b], x_recv.at[b], partner)

    def block_at(b, owner):
        return pair_in.at[b, pl.ds(owner * 2, 2)]

    def down_copy(b, dist):
        return rcopy(block_at(b, chip - dist), down_in.at[b, dist - 1], dn_send.at[b, dist - 1],
                     dn_recv.at[b, dist - 1], lane_of(chip - 1))

    def down_arrival(b, dist):
        slot = down_in.at[b, dist]
        return rcopy(slot, slot, dn_send.at[b, dist], dn_recv.at[b, dist], partner)

    def up_copy(b, dist):
        return rcopy(block_at(b, chip - dist), up_in.at[b, dist - half], up_send.at[b, dist - half],
                     up_recv.at[b, dist - half], lane_of(chip + 1))

    def up_arrival(b, dist):
        slot = up_in.at[b, dist - half - 1]
        return rcopy(slot, slot, up_send.at[b, dist - half - 1], up_recv.at[b, dist - half - 1], partner)

    def last_copy(b, dist):
        return rcopy(block_at(b, chip - dist), last_in.at[b], up_send.at[b, dist - half], last_recv.at[b],
                     lane_of(chip - dist))

    def last_arrival(b):
        slot = last_in.at[b]
        return rcopy(slot, slot, sw_send, last_recv.at[b], partner)

    def swap_copy():
        return rcopy(swap_out.at[1 - core], swap_in, sw_send, sw_recv, partner)

    far = n_chip - 1
    reach = half
    n_far = n_chip - 1 - reach

    def gather_round(when):
        for hop in range(reach + 1):
            b = when + 2 + reach - hop

            @pl.when((b >= 0) & (b < n_seq))
            def _(b=b, hop=hop):
                if hop == 0:
                    own_copy(b).start()

                    @pl.when(chip < far)
                    def _():
                        own_send(b, chip + 1, chip).start()

                    @pl.when(chip < n_far)
                    def _():
                        own_send(b, far, n_chip).start()
                    return

                @pl.when(chip >= hop)
                def _():
                    src = chip - hop
                    gather_arrival(b, src).wait_recv()
                    forward_copy(b, src).start()
                    if hop < reach:
                        @pl.when(chip < far)
                        def _():
                            pass_on(b, src, chip + 1).start()

                if hop <= n_far:
                    @pl.when(chip == n_chip - hop)
                    def _():
                        for src in range(n_far + 1 - hop):
                            gather_arrival(b, src).wait_recv()
                            forward_copy(b, src).start()
                            if src < n_far - hop:
                                pass_on(b, src, far - hop).start()

    def gather_drain(b):
        own_copy(b).wait_send()

        @pl.when(chip < far)
        def _():
            own_send(b, chip + 1, chip).wait_send()

        @pl.when(chip < n_far)
        def _():
            own_send(b, far, n_chip).wait_send()
        for hop in range(1, reach + 1):
            @pl.when(chip >= hop)
            def _(hop=hop):
                forward_copy(b, chip - hop).wait_send()
                if hop < reach:
                    @pl.when(chip < far)
                    def _():
                        pass_on(b, chip - hop, chip + 1).wait_send()
        for hop in range(1, n_far + 1):
            @pl.when(chip == n_chip - hop)
            def _(hop=hop):
                for src in range(n_far + 1 - hop):
                    forward_copy(b, src).wait_send()
                    if src < n_far - hop:
                        pass_on(b, src, far - hop).wait_send()

    @pl.when(t == 0)
    def _():
        kv_all[...] = jnp.zeros(kv_all.shape, bf16)
        doc_all[...] = jnp.zeros(doc_all.shape, jnp.int32)
        kv_all[:, pl.ds(rank, 1)] = kv_ref[...][:, None]
        doc_all[pl.ds(rank, 1)] = doc_ref[...][None]
        barrier = pltpu.get_barrier_semaphore()
        each(1, n_dev, lambda i: pl.semaphore_signal(barrier, inc=1, device_id={'cp': lax.rem(rank + i, n_dev)},
                                                     device_id_type=MESH))
        pl.semaphore_wait(barrier, n_dev - 1)
        each(rank + 1, n_dev, lambda dst: doc_copy(dst).start())

        each(-reach - 2, -1, gather_round)
        each(0, rank, lambda src: doc_arrival(src).wait_recv())
        gather_round(-1)

    def load_rows(ref, c):
        return ref[0, c * toks:(c + 1) * toks].reshape(row_block, head_dim)

    def keys_at(kb):
        return kv_all[t, pl.ds(kb * per_block, per_block), :, :head_dim].reshape(KEY_BLOCK, head_dim)

    def vals_at(kb):
        return kv_all[t, pl.ds(kb * per_block, per_block), :, head_dim:].reshape(KEY_BLOCK, head_dim)

    def score_block(kb):
        key_t = keys_at(kb).T
        doc_q = doc_col_ref[0]
        limits = []
        for p in range(KEY_BLOCK // 128):
            col = kb * KEY_BLOCK + p * 128 + lax.broadcasted_iota(jnp.int32, (piece, 128), 1)
            row = rank * piece + lax.broadcasted_iota(jnp.int32, (piece, 128), 0)
            src = kb * per_block + 2 * p
            doc_k = doc_all[src, pl.ds(t, 1)] + doc_all[src + 1, pl.ds(t, 1)]
            limits.append(jnp.where((col <= row) & (doc_q == doc_k), UNMASKED, MASKED))
        limit = jnp.concatenate(limits, axis=1)
        for c in range(n_rows):
            sl = slice(c * row_block, (c + 1) * row_block)
            raw = jnp.dot(load_rows(q_ref, c), key_t, preferred_element_type=f32)
            lim = limit[c * toks:(c + 1) * toks]
            raw = jnp.minimum((raw * base).reshape(toks, n_heads, KEY_BLOCK), lim[:, None, :]).reshape(row_block, KEY_BLOCK)
            s_scr[kb, sl, :] = raw
            old = stat_scr[sl]
            top = old
            for p in range(KEY_BLOCK // 128):
                top = jnp.maximum(top, raw[:, p * 128:(p + 1) * 128])
            total = inv_scr[sl] * jnp.exp2(old - top)
            for p in range(KEY_BLOCK // 128):
                total = total + jnp.exp2(raw[:, p * 128:(p + 1) * 128] - top)
            stat_scr[sl] = top
            inv_scr[sl] = total

    def out_block(kb, first):
        val = vals_at(kb)
        for c in range(n_rows):
            sl = slice(c * row_block, (c + 1) * row_block)
            norm = inv_scr[sl]
            parts = []
            for p in range(KEY_BLOCK // 128):
                lanes = slice(p * 128, (p + 1) * 128)
                prob = jnp.exp2(s_scr[kb, sl, lanes] - norm)
                s_scr[kb, sl, lanes] = prob
                parts.append(prob.astype(bf16))
            term = jnp.dot(jnp.concatenate(parts, axis=1), val, preferred_element_type=f32)
            acc_scr[sl] = term if first else acc_scr[sl] + term

    def grad_block(kb, first):
        key = keys_at(kb)
        val_t = vals_at(kb).T
        for c in range(n_rows):
            sl = slice(c * row_block, (c + 1) * row_block)
            gp = jnp.dot(load_rows(g_ref, c), val_t, preferred_element_type=f32)
            delta = stat_scr[sl]
            parts = []
            for p in range(KEY_BLOCK // 128):
                lanes = slice(p * 128, (p + 1) * 128)
                prob = s_scr[kb, sl, lanes]
                p_scr[sl, lanes] = prob.astype(bf16)
                parts.append((prob * (gp[:, lanes] - delta)).astype(bf16))
            ds = jnp.concatenate(parts, axis=1)
            ds_scr[sl, :] = ds
            term = jnp.dot(ds, key, preferred_element_type=f32)
            acc_scr[sl] = term if first else acc_scr[sl] + term
        dk_t = jnp.dot(qt_scr[...], ds_scr[...], preferred_element_type=f32)
        dv_t = jnp.dot(gt_scr[...], p_scr[...], preferred_element_type=f32)
        part[0, pl.ds(kb * per_block, per_block)] = dk_t.T.reshape(per_block, piece, head_dim)
        part[1, pl.ds(kb * per_block, per_block)] = dv_t.T.reshape(per_block, piece, head_dim)

    @pl.when(t < n_seq)
    def _():
        each(0, chip + 1, lambda src: forward_arrival(t, src).wait_recv())
        stat_scr[...] = jnp.full(stat_scr.shape, MASKED, f32)
        inv_scr[...] = jnp.zeros(inv_scr.shape, f32)
        each(0, hi - 1, score_block)
        for c in range(n_rows):
            sl = slice(c * row_block, (c + 1) * row_block)
            qt_scr[:, sl] = load_rows(q_ref, c).T
            gt_scr[:, sl] = load_rows(g_ref, c).T
        score_block(hi - 1)
        for c in range(n_rows):
            sl = slice(c * row_block, (c + 1) * row_block)
            old = stat_scr[sl]
            top = jnp.max(old, axis=1, keepdims=True)
            total = jnp.sum(inv_scr[sl] * jnp.exp2(old - top), axis=1, keepdims=True)
            inv_scr[sl] = jnp.broadcast_to(top + jnp.log2(total), (row_block, 128))
        out_block(hi - 1, True)


    final = half + 1

    def stage():
        for step in range(1, final + 1):
            lag = step
            live = (t >= lag) & (t < n_seq + lag)
            b = t - lag
            if step == 1:
                @pl.when(live)
                def _(b=b):
                    pair_copy(b).wait()

                    def add_own(owner):
                        sl = pl.ds(owner * 2, 2)
                        pair_in[b, sl] += part[core, sl]
                    each(0, chip + 1, add_own)
            for dist in (half + step - 1, half - step):
                if dist < 1 or dist >= n_chip:
                    continue

                @pl.when(live & (chip >= dist))
                def _(b=b, dist=dist):
                    owner = pl.ds((chip - dist) * 2, 2)
                    if dist < half:
                        if dist < half - 1:
                            @pl.when(chip < n_chip - 1)
                            def _():
                                down_arrival(b, dist).wait_recv()
                                pair_in[b, owner] += down_in[b, dist]
                        down_copy(b, dist).start()
                    else:
                        if dist > half:
                            up_arrival(b, dist).wait_recv()
                            pair_in[b, owner] += up_in[b, dist - half - 1]

                        if dist < n_chip - 1:
                            @pl.when(chip < n_chip - 1)
                            def _():
                                up_copy(b, dist).start()

                        @pl.when(chip == n_chip - 1)
                        def _():
                            last_copy(b, dist).start()
            if step == final:
                @pl.when(live)
                def _(b=b):
                    own = pl.ds(chip * 2, 2)

                    @pl.when(chip < n_chip - 1)
                    def _():
                        down_arrival(b, 0).wait_recv()
                        pair_in[b, own] += down_in[b, 0]

                    @pl.when(chip < n_chip - half)
                    def _():
                        last_arrival(b).wait_recv()
                        pair_in[b, own] += last_in[b]

                    factor = jnp.where(core == 0, scale, 1.0).astype(f32)
                    total = (pair_in[b, own] * factor).astype(bf16)
                    swap_out[0, b] = total[0]
                    swap_out[1, b] = total[1]

    stage()

    @pl.when(t < n_seq)
    def _():
        each(0, hi - 1, lambda kb: out_block(kb, False))
        for c in range(n_rows):
            sl = slice(c * row_block, (c + 1) * row_block)
            out = acc_scr[sl].astype(bf16)
            o_ref[0, c * toks:(c + 1) * toks] = out.reshape(toks, n_heads, head_dim)
            delta = jnp.sum(load_rows(g_ref, c).astype(f32) * out.astype(f32), axis=1, keepdims=True)
            stat_scr[sl] = jnp.broadcast_to(delta, (row_block, 128))
        grad_block(hi - 1, True)
        each(0, hi - 1, lambda kb: grad_block(kb, False))
        pair_copy(t).start()
        for c in range(n_rows):
            sl = slice(c * row_block, (c + 1) * row_block)
            dq_ref[0, c * toks:(c + 1) * toks] = (acc_scr[sl] * scale).astype(bf16).reshape(toks, n_heads, head_dim)

    gather_round(t)

    @pl.when(t == n_seq + final - 1)
    def _():
        swap_copy().start()
        dkv_ref[pl.ds(core, 1)] = swap_out[pl.ds(core, 1)]
        swap_copy().wait()
        dkv_ref[pl.ds(1 - core, 1)] = swap_in[...][None]
        each(rank + 1, n_dev, lambda dst: doc_copy(dst).wait_send())

        def drain(b):
            gather_drain(b)
            for dist in range(1, n_chip):
                @pl.when(chip >= dist)
                def _(dist=dist):
                    if dist < half:
                        down_copy(b, dist).wait_send()
                    else:
                        if dist < n_chip - 1:
                            @pl.when(chip < n_chip - 1)
                            def _():
                                up_copy(b, dist).wait_send()

                        @pl.when(chip == n_chip - 1)
                        def _():
                            last_copy(b, dist).wait_send()
        each(0, n_seq, drain)


def fused(query, grad_out, kv_loc, doc_send, doc_col, n_dev):
    n_seq, piece, wide = kv_loc.shape
    n_heads, head_dim = query.shape[2:]
    rows = piece * n_heads
    n_chip = n_dev // 2
    half = n_chip // 2
    seq = n_dev * piece
    f32 = jnp.float32
    bf16 = jnp.bfloat16
    tok_spec = pl.BlockSpec((1, piece, n_heads, head_dim), lambda t: (jnp.minimum(t, n_seq - 1), 0, 0, 0))
    dma = pltpu.SemaphoreType.DMA
    return pl.pallas_call(
        fused_kernel,
        grid=(n_seq + half + 1,),
        in_specs=[tok_spec, tok_spec,
                  pl.BlockSpec(memory_space=pltpu.VMEM),
                  pl.BlockSpec(memory_space=pltpu.VMEM),
                  pl.BlockSpec((1, piece, 128), lambda t: (jnp.minimum(t, n_seq - 1), 0, 0))],
        out_specs=[tok_spec, tok_spec, pl.BlockSpec(memory_space=pltpu.VMEM)],
        out_shape=[jax.ShapeDtypeStruct(query.shape, bf16),
                   jax.ShapeDtypeStruct(query.shape, bf16),
                   jax.ShapeDtypeStruct((2, n_seq, piece, head_dim), bf16)],
        scratch_shapes=[
            pltpu.VMEM((n_seq, n_dev, piece, wide), bf16),
            pltpu.VMEM((n_dev, n_seq, 128), jnp.int32),
            pltpu.VMEM((2, n_dev, piece, head_dim), f32),
            pltpu.VMEM((n_seq, n_dev, piece, head_dim), f32),
            pltpu.VMEM((n_seq, half - 1, 2, piece, head_dim), f32),
            pltpu.VMEM((n_seq, half - 1, 2, piece, head_dim), f32),
            pltpu.VMEM((n_seq, 2, piece, head_dim), f32),
            pltpu.VMEM((2, n_seq, piece, head_dim), bf16),
            pltpu.VMEM((n_seq, piece, head_dim), bf16),
            pltpu.VMEM((seq // KEY_BLOCK, rows, KEY_BLOCK), f32),
            pltpu.VMEM((rows, 128), f32),
            pltpu.VMEM((rows, 128), f32),
            pltpu.VMEM((rows, head_dim), f32),
            pltpu.VMEM((rows, KEY_BLOCK), bf16),
            pltpu.VMEM((rows, KEY_BLOCK), bf16),
            pltpu.VMEM((head_dim, rows), bf16),
            pltpu.VMEM((head_dim, rows), bf16),
            dma((n_seq, n_chip + 1)), dma((n_seq, n_chip)),
            dma((n_seq, n_chip)), dma((n_seq, n_chip)),
            dma((n_dev,)), dma((n_dev,)),
            dma((n_seq,)), dma((n_seq,)),
            dma((n_seq, half - 1)), dma((n_seq, half - 1)),
            dma((n_seq, half)), dma((n_seq, half)),
            dma((n_seq,)), dma, dma,
        ],
        compiler_params=pltpu.CompilerParams(
            collective_id=0, has_side_effects=True, vmem_limit_bytes=42 * 1024 * 1024,
            dimension_semantics=('arbitrary',)),
    )(query, grad_out, kv_loc, doc_send, doc_col)


def solution(mesh):
    n_dev = mesh.shape['cp']
    seq_spec = P('dp', 'cp', None, None)
    id_spec = P('dp', 'cp')

    def per_device(query, keys, values, grad_out, doc_id):
        n_seq, piece = doc_id.shape
        rank = lax.axis_index('cp')
        kv_loc = jnp.concatenate([keys[:, :, 0, :], values[:, :, 0, :]], axis=-1)
        blank = jnp.zeros_like(doc_id)
        doc_send = jnp.where(rank % 2 == 0, jnp.concatenate([doc_id, blank], axis=1), jnp.concatenate([blank, doc_id], axis=1))
        doc_col = jnp.broadcast_to(doc_id[:, :, None], (n_seq, piece, 128))
        out, grad_query, dkv = fused(query, grad_out, kv_loc, doc_send, doc_col, n_dev)
        return out, grad_query, dkv[0][:, :, None, :], dkv[1][:, :, None, :]

    return jax.shard_map(per_device, mesh=mesh, in_specs=(seq_spec, seq_spec, seq_spec, seq_spec, id_spec), out_specs=(seq_spec, seq_spec, seq_spec, seq_spec), check_vma=False)
```
